512 devices in a mesh: fsdp: 64 (over y, x, core), model: 8 (over z).
Axes of the slice: x: 4, y: 8, z: 8, core: 2. Of those that a mesh axis runs over, the one named last changes fastest.
Arguments:
- train_query: float32 [2560, 4096], P('fsdp', 'model'), may hold values from -0.3125 to 0.3125
- drift_query: float32 [2560, 4096], P('fsdp', 'model'), may hold values from -6 to 6
- spread_query: float32 [2560, 4096], P('fsdp', 'model'), may hold values from 0.1 to 10
- train_key: float32 [2560, 1024], P('fsdp', 'model'), may hold values from -0.3125 to 0.3125
- drift_key: float32 [2560, 1024], P('fsdp', 'model'), may hold values from -6 to 6
- spread_key: float32 [2560, 1024], P('fsdp', 'model'), may hold values from 0.1 to 10
- train_value: float32 [2560, 1024], P('fsdp', 'model'), may hold values from -0.3125 to 0.3125
- drift_value: float32 [2560, 1024], P('fsdp', 'model'), may hold values from -6 to 6
- spread_value: float32 [2560, 1024], P('fsdp', 'model'), may hold values from 0.1 to 10
- norm_train: float32 [2560], P(('fsdp', 'model')), may hold values from 0.25 to 1.75
- norm_step: float32 [2560], P(('fsdp', 'model')), may hold values from -0.3 to 0.3
Outputs:
- serve_query: bfloat16 [2560, 4096], P(None, 'model')
- serve_key: bfloat16 [2560, 1024], P(None, 'model')
- serve_value: bfloat16 [2560, 1024], P(None, 'model')
- factor_query: float32 [4096], P('model')
- factor_key: float32 [1024], P('model')
- factor_value: float32 [1024], P('model')
- serve_norm: bfloat16 [2560], replicated
- fresh_query: float32 [2560, 4096], P('fsdp', 'model')
- fresh_key: float32 [2560, 1024], P('fsdp', 'model')
- fresh_value: float32 [2560, 1024], P('fsdp', 'model')
The draws below stay inside these ranges and needn't reach their ends.
All inputs are finite; a program needn't handle non-finite values. Where the reference program divides by a largest or mean magnitude, that divisor is 1e-20 or more.
Results may differ from the reference program's by a relative error of at most 0.001.
Values may be sent and summed in bfloat16 or wider, within the bound.
No kernel may reach another device: no remote copies, remote signals or barrier semaphores. Data moves between devices by JAX's collectives and lax.ppermute only.
A program may use at most 64 MiB of HBM per device.

```python
import math
import jax
import jax.numpy as jnp
from jax import lax

D_MODEL = 2560
Q_DIM = 4096
KV_DIM = 1024


def raised(result, rng, source, target, parts, factor):
    owner, partner = [(jnp.arange(result.shape[dim]) // (result.shape[dim] // parts)).reshape([-1 if axis == dim else 1 for axis in range(result.ndim)]) for dim in (source, target)]
    chosen = jax.random.permutation(rng, parts)[partner]
    strong = (owner == chosen) | (owner == (partner + parts // 2) % parts)
    return jnp.where(strong, factor * result, result)


def block_scale(rng, dims, pieces, low, high):
    factor_of = 1.0
    for axis_at, shards_of in pieces:
        draws = jax.random.uniform(jax.random.fold_in(jax.random.fold_in(rng, 6), axis_at), (shards_of,), jnp.float32, low / len(pieces), high / len(pieces))
        factor_of = factor_of * jnp.repeat(jnp.exp(draws), dims[axis_at] // shards_of).reshape((-1,) + (1,) * (len(dims) - 1 - axis_at))
    return factor_of


def scatter_about(stream_key, extent, spread, bound, shards=(), dtype=jnp.bfloat16):
    drawn = jax.random.normal(stream_key, extent, jnp.float32) * spread
    if len(shards) > 0:
        drawn = block_scale(stream_key, extent, shards, -0.22, 0.18) * drawn
    return jnp.clip(drawn, min=-bound, max=bound).astype(dtype)


def gaussian_with(own_key, extent, deviation, limit, split, heavy, kind=jnp.bfloat16):
    entries = deviation * jax.random.normal(own_key, extent, jnp.float32)
    if split:
        entries = entries * block_scale(own_key, extent, split, -0.22, 0.18)
    return jnp.clip(raised(entries, jax.random.fold_in(own_key, 3), *heavy), -limit, limit).astype(kind)


def setup_inputs(seed: int = 0) -> dict:
    arg_keys = jax.random.split(jax.random.key(seed), 12)
    train_query = gaussian_with(arg_keys[0], (D_MODEL, Q_DIM), D_MODEL ** -0.5, 0.3125, ((0, 64), (1, 8)), (0, 1, 64, 4.0), jnp.float32)
    drift_query = scatter_about(arg_keys[1], (D_MODEL, Q_DIM), 1.0, 6.0, ((0, 64), (1, 8)), jnp.float32)
    spread_query = jnp.clip(jnp.exp(math.log(10.0) - 4.6051702 * jax.random.uniform(arg_keys[2], (D_MODEL, Q_DIM), jnp.float32) ** block_scale(arg_keys[2], (D_MODEL, Q_DIM), ((0, 64), (1, 8)), -0.2, 0.2)), 0.1, 10.0)
    train_key = gaussian_with(arg_keys[3], (D_MODEL, KV_DIM), D_MODEL ** -0.5, 0.3125, ((0, 64), (1, 8)), (0, 1, 64, 4.0), jnp.float32)
    drift_key = scatter_about(arg_keys[4], (D_MODEL, KV_DIM), 1.0, 6.0, ((0, 64), (1, 8)), jnp.float32)
    spread_key = jnp.clip(jnp.exp(math.log(10.0) - 4.6051702 * jax.random.uniform(arg_keys[5], (D_MODEL, KV_DIM), jnp.float32) ** block_scale(arg_keys[5], (D_MODEL, KV_DIM), ((0, 64), (1, 8)), -0.2, 0.2)), 0.1, 10.0)
    train_value = gaussian_with(arg_keys[6], (D_MODEL, KV_DIM), D_MODEL ** -0.5, 0.3125, ((0, 64), (1, 8)), (0, 1, 64, 4.0), jnp.float32)
    drift_value = scatter_about(arg_keys[7], (D_MODEL, KV_DIM), 1.0, 6.0, ((0, 64), (1, 8)), jnp.float32)
    spread_value = jnp.clip(jnp.exp(math.log(10.0) - 4.6051702 * jax.random.uniform(arg_keys[8], (D_MODEL, KV_DIM), jnp.float32) ** block_scale(arg_keys[8], (D_MODEL, KV_DIM), ((0, 64), (1, 8)), -0.2, 0.2)), 0.1, 10.0)
    norm_train = jnp.clip(1.0 + 0.15 * jax.random.normal(arg_keys[9], (D_MODEL,), jnp.float32), 0.25, 1.75)
    norm_step = jnp.clip(jax.random.uniform(arg_keys[10], (D_MODEL,), jnp.float32, -0.3, 0.3) * block_scale(arg_keys[10], (D_MODEL,), ((0, 512),), -0.4, 0.0), -0.3, 0.3)
    return dict(train_query=train_query, drift_query=drift_query, spread_query=spread_query, train_key=train_key, drift_key=drift_key, spread_key=spread_key, train_value=train_value, drift_value=drift_value, spread_value=spread_value, norm_train=norm_train, norm_step=norm_step)


learn_rate = 0.02
decay_rate = 0.05
tiny_value = 1e-08

def reference(train_query, drift_query, spread_query, train_key, drift_key, spread_key, train_value, drift_value, spread_value, norm_train, norm_step):
    fresh_query = train_query - learn_rate * (drift_query / (jnp.sqrt(spread_query) + tiny_value) + decay_rate * train_query)
    fresh_key = train_key - learn_rate * (drift_key / (jnp.sqrt(spread_key) + tiny_value) + decay_rate * train_key)
    fresh_value = train_value - learn_rate * (drift_value / (jnp.sqrt(spread_value) + tiny_value) + decay_rate * train_value)
    factor_query = lax.optimization_barrier(jnp.max(jnp.abs(fresh_query), axis=0))
    serve_query = (fresh_query / factor_query).astype(jnp.bfloat16)
    factor_key = lax.optimization_barrier(jnp.max(jnp.abs(fresh_key), axis=0))
    serve_key = (fresh_key / factor_key).astype(jnp.bfloat16)
    factor_value = lax.optimization_barrier(jnp.max(jnp.abs(fresh_value), axis=0))
    serve_value = (fresh_value / factor_value).astype(jnp.bfloat16)
    serve_norm = (norm_train + norm_step).astype(jnp.bfloat16)
    return (serve_query, serve_key, serve_value, factor_query, factor_key, factor_value, serve_norm, fresh_query, fresh_key, fresh_value)
```

```python
import functools

import jax
import jax.numpy as jnp
from jax import lax
from jax.experimental import pallas as pl
from jax.experimental.pallas import tpu as pltpu
from jax.sharding import Mesh
from jax.sharding import PartitionSpec as P


Y, X, C, Z = "fsdp_0", "fsdp_1", "fsdp_2", "model"
FSDP = (Y, X, C)
NY, NX = 8, 4

learn_rate = 0.02
decay_rate = 0.05
tiny_value = 1e-08

LANES = 128
SPAN = 250.0
FLOOR = 1e-28
PARTS = 3


def padded(rows):
    return -(-rows // 8) * 8


def encode_kernel(widths, where_ref, norm_train, norm_step, *refs):
    n = len(widths)
    ins, fresh_refs, wire = refs[: 3 * n], refs[3 * n : 4 * n], refs[4 * n]
    copies = wire.shape[0]
    rows = ins[0].shape[0]
    slabs = sum(w // LANES for w in widths)
    slab = 0
    for at, width in enumerate(widths):
        train, drift, spread = ins[3 * at : 3 * at + 3]
        for k in range(width // LANES):
            cols = slice(k * LANES, (k + 1) * LANES)
            t = train[:, cols]
            fresh = t - learn_rate * (
                drift[:, cols] / (jnp.sqrt(spread[:, cols]) + tiny_value) + decay_rate * t
            )
            fresh_refs[at][:, cols] = fresh
            size = jnp.abs(fresh)
            scale = jnp.maximum(jnp.max(size, axis=0, keepdims=True), FLOOR)
            code = jnp.exp2(size * (SPAN / scale) - SPAN / 2)
            code = jnp.where(fresh < 0, -code, code).astype(jnp.bfloat16)
            left = scale
            parts = []
            for _ in range(PARTS):
                part = left.astype(jnp.bfloat16)
                parts.append(part)
                left = left - part.astype(jnp.float32)
            for c in range(copies):
                wire[c, slab * rows : (slab + 1) * rows, :] = code
                for p, part in enumerate(parts):
                    row = slabs * rows + p * slabs + slab
                    wire[c, row : row + 1, :] = part
            slab += 1
    used = slabs * (rows + PARTS)
    few = norm_train.shape[0]
    lane = lax.broadcasted_iota(jnp.int32, (1, LANES), 1) - where_ref[2] * few
    gain = jnp.zeros((1, LANES), jnp.float32)
    for i in range(few):
        gain = jnp.where(lane == i, norm_train[i] + norm_step[i], gain)
    gain = gain.astype(jnp.bfloat16)
    for c in range(copies):
        wire[c, used : used + 1, :] = gain
        if used + 1 < wire.shape[1]:
            wire[c, used + 1 :, :] = jnp.zeros((wire.shape[1] - used - 1, LANES), jnp.bfloat16)


def encode(copies, where, norms, arrays):
    rows = arrays[0].shape[0]
    widths = tuple(a.shape[1] for a in arrays[::3])
    slabs = sum(w // LANES for w in widths)
    out = [jax.ShapeDtypeStruct(a.shape, a.dtype) for a in arrays[::3]]
    out.append(
        jax.ShapeDtypeStruct((copies, padded(slabs * (rows + PARTS) + 1), LANES), jnp.bfloat16)
    )
    vmem = pl.BlockSpec(memory_space=pltpu.VMEM)
    smem = pl.BlockSpec(memory_space=pltpu.SMEM)
    return pl.pallas_call(
        functools.partial(encode_kernel, widths),
        out_shape=out,
        in_specs=[smem] * 3 + [vmem] * len(arrays),
        out_specs=[vmem] * len(out),
        name="encode",
    )(where, *norms, *arrays)


def decode_kernel(widths, rows, where_ref, *refs):
    n = len(widths)
    wires, gains = refs[:8], refs[8]
    serve, factor, norm = refs[9 : 9 + n], refs[9 + n : 9 + 2 * n], refs[9 + 2 * n]
    scratch = refs[10 + 2 * n :]
    stage, ratios, sems = scratch[:n], scratch[n], scratch[n + 1]
    slabs = sum(w // LANES for w in widths)
    low = slabs * rows
    mine, kind = where_ref[0], where_ref[1]
    best = None
    for i, wire in enumerate(wires):
        tail = wire[:, low:, :].astype(jnp.float32)
        scale = tail[:, :slabs]
        for p in range(1, PARTS):
            scale = scale + tail[:, p * slabs : (p + 1) * slabs]
        ratios[i] = scale
        top = jnp.max(scale, axis=0)
        best = top if best is None else jnp.maximum(best, top)
    slab = 0
    for at, width in enumerate(widths):
        for k in range(width // LANES):
            factor[at][:, k * LANES : (k + 1) * LANES] = best[slab : slab + 1]
            slab += 1
    share = 1.0 / (SPAN * best)
    for i in range(8):
        ratios[i] = ratios[i] * share

    def copy(at, y):
        return pltpu.make_async_copy(stage[at].at[y], serve[at].at[y], sems.at[at, y])

    def body(y, _):
        for i, wire in enumerate(wires):
            x = lax.rem(kind + i % 4 + 2 * y, NX)
            c = mine if i < 4 else 1 - mine
            slab = 0
            for at, width in enumerate(widths):
                for k in range(width // LANES):
                    cols = slice(k * LANES, (k + 1) * LANES)
                    code = wire[y, slab * rows : (slab + 1) * rows, :].astype(jnp.float32)
                    ratio = ratios[i, y, slab : slab + 1, :]
                    size = (jnp.log2(jnp.abs(code)) + SPAN / 2) * ratio
                    stage[at][y, x, c, :, cols] = jnp.where(code < 0, -size, size).astype(
                        jnp.bfloat16
                    )
                    slab += 1
        for at in range(n):
            copy(at, y).start()
        return 0

    lax.fori_loop(0, NY, body, 0)
    few = norm.shape[1]
    for k in range(NX):
        for c in range(2):
            total = jnp.sum(gains[k, c].astype(jnp.float32), axis=0)
            for y in range(NY):
                x = (k + 2 * y) % NX
                row = (y * NX + x) * 2 + c
                norm[row : row + 1, :] = total[y : y + 1, :few]
    for at in range(n):
        for y in range(NY):
            copy(at, y).wait()


def decode(widths, rows, few, where, wires, gains):
    stage = [(NY, NX, 2, rows, w) for w in widths]
    vmem = pl.BlockSpec(memory_space=pltpu.VMEM)
    slabs = sum(w // LANES for w in widths)
    out = [jax.ShapeDtypeStruct(s, jnp.bfloat16) for s in stage]
    out += [jax.ShapeDtypeStruct((1, w), jnp.float32) for w in widths]
    out.append(jax.ShapeDtypeStruct((NY * NX * 2, few), jnp.float32))
    return pl.pallas_call(
        functools.partial(decode_kernel, widths, rows),
        out_shape=out,
        in_specs=[pl.BlockSpec(memory_space=pltpu.SMEM)] + [vmem] * 9,
        out_specs=[pl.BlockSpec(memory_space=pl.ANY)] * len(widths) + [vmem] * (len(widths) + 1),
        scratch_shapes=[pltpu.VMEM(s, jnp.bfloat16) for s in stage]
        + [
            pltpu.VMEM((8, NY, slabs, LANES), jnp.float32),
            pltpu.SemaphoreType.DMA((len(widths), NY)),
        ],
        name="decode",
    )(where, *wires, gains)


def place(y, x, c):
    return ((y % NY) * NX + x % NX) * 2 + c


SPOTS = [(y, x, c) for y in range(NY) for x in range(NX) for c in range(2)]


def come_from(value, source):
    return lax.ppermute(value, FSDP, [(place(*source(*s)), place(*s)) for s in SPOTS])


def per_device(n_z, *args):
    arrays, norms = args[:9], args[9:]
    rows = arrays[0].shape[0]
    widths = tuple(a.shape[1] for a in arrays[::3])
    y, x, c, z = (lax.axis_index(a).astype(jnp.int32) for a in (Y, X, C, Z))
    where = jnp.stack([c, (x + 2 * y) % NX, z])
    *fresh, wire = encode(NY, where, norms, arrays)
    same_kind = [[place(y, k - 2 * y, c) for y in range(NY)] for c in range(2) for k in range(NX)]
    own = lax.all_to_all(wire, FSDP, 0, 0, axis_index_groups=same_kind, tiled=True)

    up = come_from(own, lambda y, x, c: (y, x + 1, c))
    down = come_from(own, lambda y, x, c: (y, x - 1, c))
    side = come_from(own, lambda y, x, c: (y + 1 - 2 * c, x, c))
    side_other = come_from(own, lambda y, x, c: (y - 1 + 2 * c, x, 1 - c))
    swap = lambda v: come_from(v, lambda y, x, c: (y, x, 1 - c))
    own_other = swap(own)

    used = sum(w // LANES for w in widths) * (rows + PARTS)
    gain = jnp.broadcast_to(own[:, used, :][None], (NX * 2 * n_z, NY, LANES))
    rest = [
        [(place(y, k - 2 * y, c) * n_z) + z for k in range(NX) for c in range(2) for z in range(n_z)]
        for y in range(NY)
    ]
    gains = lax.all_to_all(gain, FSDP + (Z,), 0, 0, axis_index_groups=rest, tiled=True)
    gains = gains.reshape(NX, 2, n_z, NY, LANES)

    wires = (own, up, side, down, own_other, swap(up), side_other, swap(down))
    few = norms[0].shape[0] * n_z
    out = decode(widths, rows, few, where, wires, gains)
    serve = [s.reshape(-1, s.shape[-1]) for s in out[:3]]
    factor = [f.reshape(-1) for f in out[3:6]]
    return (*serve, *factor, out[6].astype(jnp.bfloat16).reshape(-1), *fresh)


def solution(mesh):
    split = Mesh(mesh.devices.reshape(NY, NX, 2, mesh.shape["model"]), (Y, X, C, Z))
    return jax.shard_map(
        functools.partial(per_device, mesh.shape["model"]),
        mesh=split,
        in_specs=(P(FSDP, Z),) * 9 + (P((*FSDP, Z)),) * 2,
        out_specs=(P(None, Z),) * 3 + (P(Z),) * 3 + (P(),) + (P(FSDP, Z),) * 3,
        check_vma=False,
    )
```

```python
import functools

import jax
import jax.numpy as jnp
from jax import lax
from jax.experimental import pallas as pl
from jax.experimental.pallas import tpu as pltpu
from jax.sharding import Mesh
from jax.sharding import PartitionSpec as P


Y, X, C, Z = "fsdp_0", "fsdp_1", "fsdp_2", "model"
FSDP = (Y, X, C)
NY, NX = 8, 4

learn_rate = 0.02
decay_rate = 0.05
tiny_value = 1e-08

LANES = 128
SPAN = 125.0
FLOOR = 1e-28
PARTS = 2


def padded(rows):
    return -(-rows // 8) * 8


def spot():
    return tuple(lax.axis_index(a) for a in (Y, X, C))


def encode_kernel(widths, norm_train, norm_step, *refs):
    n = len(widths)
    sources, fresh_refs, wire = refs[: 3 * n], refs[3 * n : 4 * n], refs[4 * n]
    ins, sems = refs[4 * n + 1 : -1], refs[-1]
    loads = [pltpu.make_async_copy(s, d, sems.at[i]) for i, (s, d) in enumerate(zip(sources, ins))]
    for load in loads:
        load.start()
    copies = wire.shape[0]
    rows = ins[0].shape[0]
    slabs = sum(w // LANES for w in widths)
    slab = 0
    for at, width in enumerate(widths):
        train, drift, spread = ins[3 * at : 3 * at + 3]
        for load in loads[3 * at : 3 * at + 3]:
            load.wait()
        for k in range(width // LANES):
            cols = slice(k * LANES, (k + 1) * LANES)
            t = train[:, cols]
            fresh = t - learn_rate * (
                drift[:, cols] / (jnp.sqrt(spread[:, cols]) + tiny_value) + decay_rate * t
            )
            fresh_refs[at][:, cols] = fresh
            left = jnp.maximum(jnp.max(jnp.abs(fresh), axis=0, keepdims=True), FLOOR)
            parts = []
            scale = jnp.zeros_like(left)
            for _ in range(PARTS):
                parts.append(left.astype(jnp.bfloat16))
                part = parts[-1].astype(jnp.float32)
                scale, left = scale + part, left - part
            code = jnp.exp2(fresh * (SPAN / scale)).astype(jnp.bfloat16)
            for c in range(copies):
                wire[c, slab * rows : (slab + 1) * rows, :] = code
                for p, part in enumerate(parts):
                    row = slabs * rows + p * slabs + slab
                    wire[c, row : row + 1, :] = part
            slab += 1
    used = slabs * (rows + PARTS)
    few = norm_train.shape[0]
    y, x, c = spot()
    start = (place(y, x, c) * lax.axis_size(Z) + lax.axis_index(Z)) * few
    lane = lax.broadcasted_iota(jnp.int32, (1, LANES), 1) - lax.rem(start, LANES)
    lane = jnp.where(lane < 0, lane + LANES, lane)
    gain = jnp.zeros((1, LANES), jnp.float32)
    for i in range(few):
        gain = jnp.where(lane == i, norm_train[i] + norm_step[i], gain)
    gain = gain.astype(jnp.bfloat16)
    for copy in range(copies):
        wire[copy, used : used + 1, :] = gain


def encode(copies, norms, arrays):
    rows = arrays[0].shape[0]
    widths = tuple(a.shape[1] for a in arrays[::3])
    slabs = sum(w // LANES for w in widths)
    out = [pltpu.VMEM(a.shape, a.dtype) for a in arrays[::3]]
    out.append(pltpu.VMEM((copies, padded(slabs * (rows + PARTS) + 1), LANES), jnp.bfloat16))
    vmem = pl.BlockSpec(memory_space=pltpu.VMEM)
    return pl.pallas_call(
        functools.partial(encode_kernel, widths),
        out_shape=out,
        in_specs=[pl.BlockSpec(memory_space=pltpu.SMEM)] * 2
        + [pl.BlockSpec(memory_space=pltpu.HBM)] * len(arrays),
        out_specs=[vmem] * len(out),
        scratch_shapes=[pltpu.VMEM(a.shape, a.dtype) for a in arrays]
        + [pltpu.SemaphoreType.DMA((len(arrays),))],
        compiler_params=pltpu.CompilerParams(vmem_limit_bytes=16 * 2**20),
        name="encode",
    )(*(in_hbm(a) for a in norms), *(in_hbm(a) for a in arrays))


def prepare_kernel(row, own, out):
    rows = own[:, row - row % 8 : row - row % 8 + 8, :].astype(jnp.float32)[:, row % 8, :]
    rows = rows.astype(out.dtype)
    for i in range(out.shape[0]):
        out[i] = rows


def prepare(row, copies, own):
    vmem = pl.BlockSpec(memory_space=pltpu.VMEM)
    return pl.pallas_call(
        functools.partial(prepare_kernel, row),
        out_shape=pltpu.VMEM((copies, own.shape[0], LANES), own.dtype),
        in_specs=[vmem],
        out_specs=vmem,
        compiler_params=pltpu.CompilerParams(vmem_limit_bytes=4 * 2**20),
        name="prepare",
    )(in_vmem(own))


def pack_kernel(*refs):
    for i, ref in enumerate(refs[:-1]):
        refs[-1][i] = ref[...]


def pack(arrays):
    vmem = pl.BlockSpec(memory_space=pltpu.VMEM)
    return pl.pallas_call(
        pack_kernel,
        out_shape=pltpu.VMEM((len(arrays), *arrays[0].shape), arrays[0].dtype),
        in_specs=[vmem] * len(arrays),
        out_specs=vmem,
        compiler_params=pltpu.CompilerParams(vmem_limit_bytes=4 * 2**20),
        name="pack",
    )(*(in_vmem(a) for a in arrays))


def in_hbm(value):
    return pltpu.with_memory_space_constraint(value, pltpu.HBM)


def in_vmem(value):
    return pltpu.with_memory_space_constraint(value, pltpu.VMEM)


def decode_kernel(widths, rows, *refs):
    n = len(widths)
    wires = [refs[i // 4].at[i % 4] for i in range(8)]
    refs = refs[2:]
    serve, factor, scratch = refs[:n], refs[n : 2 * n], refs[2 * n :]
    stage, ratios, sems = scratch[:n], scratch[n], scratch[n + 1]
    slabs = sum(w // LANES for w in widths)
    low = slabs * rows
    y, x, mine = spot()
    kind = lax.rem(x + 2 * y, NX)
    best = None
    for i, wire in enumerate(wires):
        tail = wire[:, low:, :].astype(jnp.float32)
        scale = tail[:, :slabs]
        for p in range(1, PARTS):
            scale = scale + tail[:, p * slabs : (p + 1) * slabs]
        ratios[i] = scale
        top = jnp.max(scale, axis=0)
        best = top if best is None else jnp.maximum(best, top)
    slab = 0
    for at, width in enumerate(widths):
        for k in range(width // LANES):
            factor[at][:, k * LANES : (k + 1) * LANES] = best[slab : slab + 1]
            slab += 1
    share = 1.0 / (SPAN * best)
    for i in range(8):
        ratios[i] = ratios[i] * share

    def copy(at, y):
        return pltpu.make_async_copy(stage[at].at[y], serve[at].at[y], sems.at[at, y])

    def body(y, _):
        for i, wire in enumerate(wires):
            x = lax.rem(kind + i % 4 + 2 * y, NX)
            c = mine if i < 4 else 1 - mine
            slab = 0
            for at, width in enumerate(widths):
                for k in range(width // LANES):
                    cols = slice(k * LANES, (k + 1) * LANES)
                    code = wire[y, slab * rows : (slab + 1) * rows, :].astype(jnp.float32)
                    ratio = ratios[i, y, slab : slab + 1, :]
                    stage[at][y, x, c, :, cols] = (jnp.log2(code) * ratio).astype(jnp.bfloat16)
                    slab += 1
        for at in range(n):
            copy(at, y).start()
        return 0

    lax.fori_loop(0, NY, body, 0)
    for at in range(n):
        for y in range(NY):
            copy(at, y).wait()


def decode(widths, rows, own, other):
    stage = [(NY, NX, 2, rows, w) for w in widths]
    vmem = pl.BlockSpec(memory_space=pltpu.VMEM)
    slabs = sum(w // LANES for w in widths)
    out = [jax.ShapeDtypeStruct(s, jnp.bfloat16) for s in stage]
    out += [jax.ShapeDtypeStruct((1, w), jnp.float32) for w in widths]
    return pl.pallas_call(
        functools.partial(decode_kernel, widths, rows),
        out_shape=out,
        in_specs=[vmem] * 2,
        out_specs=[pl.BlockSpec(memory_space=pl.ANY)] * len(widths) + [vmem] * len(widths),
        scratch_shapes=[pltpu.VMEM(s, jnp.bfloat16) for s in stage]
        + [
            pltpu.VMEM((8, NY, slabs, LANES), jnp.float32),
            pltpu.SemaphoreType.DMA((len(widths), NY)),
        ],
        compiler_params=pltpu.CompilerParams(vmem_limit_bytes=16 * 2**20),
        name="decode",
    )(in_vmem(own), in_vmem(other))


def norm_kernel(gains, _, norm):
    few = norm.shape[0] * LANES // (NY * NX * 2)
    row = lax.broadcasted_iota(jnp.int32, (padded(norm.shape[0]), NY), 0)
    chip = lax.broadcasted_iota(jnp.int32, (padded(norm.shape[0]), NY), 1)
    lane = lax.broadcasted_iota(jnp.int32, (NY, LANES), 1)
    own_y = lax.broadcasted_iota(jnp.int32, (NY, LANES), 0)
    total = jnp.zeros((padded(norm.shape[0]), LANES), jnp.float32)
    for k in range(NX):
        for c in range(2):
            start = lambda y: ((y * NX + lax.rem(k + 2 * y, NX)) * 2 + c) * few
            values = jnp.sum(gains[k, c].astype(jnp.float32), axis=0)
            here = lane >= lax.rem(start(own_y), LANES)
            for j in range(2):
                part = jnp.where(here if j == 0 else ~here, values, 0.0).astype(jnp.bfloat16)
                pick = jnp.where(lax.div(start(chip), LANES) + j == row, 1.0, 0.0)
                total = total + jnp.dot(
                    pick.astype(jnp.bfloat16), part, preferred_element_type=jnp.float32
                )
    norm[...] = total[: norm.shape[0]].astype(norm.dtype)


def gather_norm(few, gains, after):
    return pl.pallas_call(
        norm_kernel,
        out_shape=jax.ShapeDtypeStruct((NY * NX * 2 * few // LANES, LANES), jnp.bfloat16),
        in_specs=[pl.BlockSpec(memory_space=pltpu.VMEM)] * 2,
        out_specs=pl.BlockSpec(memory_space=pltpu.VMEM),
        compiler_params=pltpu.CompilerParams(vmem_limit_bytes=4 * 2**20),
        name="gather_norm",
    )(gains, after)


def place(y, x, c):
    return ((y % NY) * NX + x % NX) * 2 + c


SPOTS = [(y, x, c) for y in range(NY) for x in range(NX) for c in range(2)]


def come_from(value, source):
    return lax.ppermute(value, FSDP, [(place(*source(*s)), place(*s)) for s in SPOTS])


def per_device(n_z, *args):
    arrays, norms = args[:9], args[9:]
    rows = arrays[0].shape[0]
    widths = tuple(a.shape[1] for a in arrays[::3])
    *fresh, wire = encode(NY, norms, arrays)
    same_kind = [[place(y, k - 2 * y, c) for y in range(NY)] for c in range(2) for k in range(NX)]
    own = lax.all_to_all(wire, FSDP, 0, 0, axis_index_groups=same_kind, tiled=True)
    up = come_from(own, lambda y, x, c: (y, x + 1, c))
    down = come_from(own, lambda y, x, c: (y, x - 1, c))
    side = come_from(own, lambda y, x, c: (y + 1 - 2 * c, x, c))
    used = sum(w // LANES for w in widths) * (rows + PARTS)
    gain = prepare(used, NX * 2 * n_z, own)
    rest = [
        [
            (place(y, k - 2 * y, c) * n_z) + z
            for k in range(NX)
            for c in range(2)
            for z in range(n_z)
        ]
        for y in range(NY)
    ]
    gains = lax.all_to_all(gain, FSDP + (Z,), 0, 0, axis_index_groups=rest, tiled=True)
    gains = gains.reshape(NX, 2, n_z, NY, LANES)
    own = pack((own, up, side, down))
    other = come_from(own, lambda y, x, c: (y, x, 1 - c))

    out = decode(widths, rows, own, other)
    norm = gather_norm(norms[0].shape[0] * n_z, gains, out[3])
    serve = [s.reshape(-1, s.shape[-1]) for s in out[:3]]
    factor = [f.reshape(-1) for f in out[3:]]
    return (*serve, *factor, norm.reshape(-1), *fresh)


def solution(mesh):
    split = Mesh(mesh.devices.reshape(NY, NX, 2, mesh.shape["model"]), (Y, X, C, Z))
    return jax.shard_map(
        functools.partial(per_device, mesh.shape["model"]),
        mesh=split,
        in_specs=(P(FSDP, Z),) * 9 + (P((*FSDP, Z)),) * 2,
        out_specs=(P(None, Z),) * 3 + (P(Z),) * 3 + (P(),) + (P(FSDP, Z),) * 3,
        check_vma=False,
    )
```

```python
import functools

import jax
import jax.numpy as jnp
from jax import lax
from jax.experimental import pallas as pl
from jax.experimental.pallas import tpu as pltpu
from jax.sharding import Mesh
from jax.sharding import PartitionSpec as P


Y, X, C, Z = "fsdp_0", "fsdp_1", "fsdp_2", "model"
FSDP = (Y, X, C)
NY, NX = 8, 4

learn_rate = 0.02
decay_rate = 0.05
tiny_value = 1e-08

LANES = 128
SPAN = 125.0
FLOOR = 1e-28
PARTS = 2


def padded(rows):
    return -(-rows // 8) * 8


def spot():
    return tuple(lax.axis_index(a) for a in (Y, X, C))


def encode_kernel(widths, *refs):
    n = len(widths)
    norms, refs = refs[:2], refs[2:]
    sources, fresh_refs, wire = refs[: 3 * n], refs[3 * n : 4 * n], refs[4 * n]
    ins, (norm_train, norm_step, sems) = refs[4 * n + 1 : -3], refs[-3:]
    loads = [pltpu.make_async_copy(s, d, sems.at[i]) for i, (s, d) in enumerate(zip(sources, ins))]
    few_loads = [
        pltpu.make_async_copy(s, d, sems.at[3 * n + i])
        for i, (s, d) in enumerate(zip(norms, (norm_train, norm_step)))
    ]
    for load in loads + few_loads:
        load.start()
    copies = wire.shape[0]
    rows = ins[0].shape[0]
    slabs = sum(w // LANES for w in widths)
    slab = 0
    for at, width in enumerate(widths):
        train, drift, spread = ins[3 * at : 3 * at + 3]
        for load in loads[3 * at : 3 * at + 3]:
            load.wait()
        for k in range(width // LANES):
            cols = slice(k * LANES, (k + 1) * LANES)
            t = train[:, cols]
            fresh = t - learn_rate * (
                drift[:, cols] / (jnp.sqrt(spread[:, cols]) + tiny_value) + decay_rate * t
            )
            fresh_refs[at][:, cols] = fresh
            left = jnp.maximum(jnp.max(jnp.abs(fresh), axis=0, keepdims=True), FLOOR)
            parts = []
            scale = jnp.zeros_like(left)
            for _ in range(PARTS):
                parts.append(left.astype(jnp.bfloat16))
                part = parts[-1].astype(jnp.float32)
                scale, left = scale + part, left - part
            code = jnp.exp2(fresh * (SPAN / scale)).astype(jnp.bfloat16)
            for c in range(copies):
                wire[c, slab * rows : (slab + 1) * rows, :] = code
                for p, part in enumerate(parts):
                    row = slabs * rows + p * slabs + slab
                    wire[c, row : row + 1, :] = part
            slab += 1
    used = slabs * (rows + PARTS)
    few = norm_train.shape[0]
    y, x, c = spot()
    start = (place(y, x, c) * lax.axis_size(Z) + lax.axis_index(Z)) * few
    lane = lax.broadcasted_iota(jnp.int32, (1, LANES), 1) - lax.rem(start, LANES)
    lane = jnp.where(lane < 0, lane + LANES, lane)
    gain = jnp.zeros((1, LANES), jnp.float32)
    for load in few_loads:
        load.wait()
    for i in range(few):
        gain = jnp.where(lane == i, norm_train[i] + norm_step[i], gain)
    gain = gain.astype(jnp.bfloat16)
    for copy in range(copies):
        wire[copy, used : used + 1, :] = gain


def encode(copies, norms, arrays):
    rows = arrays[0].shape[0]
    widths = tuple(a.shape[1] for a in arrays[::3])
    slabs = sum(w // LANES for w in widths)
    out = [pltpu.VMEM(a.shape, a.dtype) for a in arrays[::3]]
    out.append(pltpu.VMEM((copies, padded(slabs * (rows + PARTS) + 1), LANES), jnp.bfloat16))
    vmem = pl.BlockSpec(memory_space=pltpu.VMEM)
    return pl.pallas_call(
        functools.partial(encode_kernel, widths),
        out_shape=out,
        in_specs=[pl.BlockSpec(memory_space=pltpu.HBM)] * (2 + len(arrays)),
        out_specs=[vmem] * len(out),
        scratch_shapes=[pltpu.VMEM(a.shape, a.dtype) for a in arrays]
        + [pltpu.SMEM(a.shape, a.dtype) for a in norms]
        + [pltpu.SemaphoreType.DMA((len(arrays) + 2,))],
        compiler_params=pltpu.CompilerParams(vmem_limit_bytes=16 * 2**20),
        name="encode",
    )(*(in_hbm(a) for a in norms), *(in_hbm(a) for a in arrays))


def prepare_kernel(row, own, out):
    rows = own[:, row - row % 8 : row - row % 8 + 8, :].astype(jnp.float32)[:, row % 8, :]
    rows = rows.astype(out.dtype)
    for i in range(out.shape[0]):
        out[i] = rows


def prepare(row, copies, own):
    vmem = pl.BlockSpec(memory_space=pltpu.VMEM)
    return pl.pallas_call(
        functools.partial(prepare_kernel, row),
        out_shape=pltpu.VMEM((copies, own.shape[0], LANES), own.dtype),
        in_specs=[vmem],
        out_specs=vmem,
        compiler_params=pltpu.CompilerParams(vmem_limit_bytes=4 * 2**20),
        name="prepare",
    )(in_vmem(own))


def pack_kernel(*refs):
    for i, ref in enumerate(refs[:-1]):
        refs[-1][i] = ref[...]


def pack(arrays):
    vmem = pl.BlockSpec(memory_space=pltpu.VMEM)
    return pl.pallas_call(
        pack_kernel,
        out_shape=pltpu.VMEM((len(arrays), *arrays[0].shape), arrays[0].dtype),
        in_specs=[vmem] * len(arrays),
        out_specs=vmem,
        compiler_params=pltpu.CompilerParams(vmem_limit_bytes=4 * 2**20),
        name="pack",
    )(*(in_vmem(a) for a in arrays))


def in_hbm(value):
    return pltpu.with_memory_space_constraint(value, pltpu.HBM)


def in_vmem(value):
    return pltpu.with_memory_space_constraint(value, pltpu.VMEM)


def decode_kernel(widths, rows, *refs):
    n = len(widths)
    wires = [refs[i // 4].at[i % 4] for i in range(8)]
    refs = refs[2:]
    serve, factor, scratch = refs[:n], refs[n : 2 * n], refs[2 * n :]
    stage, ratios, sems = scratch[:n], scratch[n], scratch[n + 1]
    slabs = sum(w // LANES for w in widths)
    low = slabs * rows
    y, x, mine = spot()
    kind = lax.rem(x + 2 * y, NX)
    best = None
    for i, wire in enumerate(wires):
        tail = wire[:, low:, :].astype(jnp.float32)
        scale = tail[:, :slabs]
        for p in range(1, PARTS):
            scale = scale + tail[:, p * slabs : (p + 1) * slabs]
        ratios[i] = scale
        top = jnp.max(scale, axis=0)
        best = top if best is None else jnp.maximum(best, top)
    slab = 0
    for at, width in enumerate(widths):
        for k in range(width // LANES):
            factor[at][:, k * LANES : (k + 1) * LANES] = best[slab : slab + 1]
            slab += 1
    share = 1.0 / (SPAN * best)
    for i in range(8):
        ratios[i] = ratios[i] * share

    def copy(at, y):
        return pltpu.make_async_copy(stage[at].at[y], serve[at].at[y], sems.at[at, y])

    def body(y, _):
        for i, wire in enumerate(wires):
            c = mine if i < 4 else 1 - mine
            x = lax.rem(kind + (0, 1 + 2 * c, 2, 3 - 2 * c)[i % 4] + 2 * y, NX)
            slab = 0
            for at, width in enumerate(widths):
                for k in range(width // LANES):
                    cols = slice(k * LANES, (k + 1) * LANES)
                    code = wire[y, slab * rows : (slab + 1) * rows, :].astype(jnp.float32)
                    ratio = ratios[i, y, slab : slab + 1, :]
                    stage[at][y, x, c, :, cols] = (jnp.log2(code) * ratio).astype(jnp.bfloat16)
                    slab += 1
        for at in range(n):
            copy(at, y).start()
        return 0

    lax.fori_loop(0, NY, body, 0)
    for at in range(n):
        for y in range(NY):
            copy(at, y).wait()


def decode(widths, rows, own, other):
    stage = [(NY, NX, 2, rows, w) for w in widths]
    vmem = pl.BlockSpec(memory_space=pltpu.VMEM)
    slabs = sum(w // LANES for w in widths)
    out = [jax.ShapeDtypeStruct(s, jnp.bfloat16) for s in stage]
    out += [jax.ShapeDtypeStruct((1, w), jnp.float32) for w in widths]
    return pl.pallas_call(
        functools.partial(decode_kernel, widths, rows),
        out_shape=out,
        in_specs=[vmem] * 2,
        out_specs=[pl.BlockSpec(memory_space=pl.ANY)] * len(widths) + [vmem] * len(widths),
        scratch_shapes=[pltpu.VMEM(s, jnp.bfloat16) for s in stage]
        + [
            pltpu.VMEM((8, NY, slabs, LANES), jnp.float32),
            pltpu.SemaphoreType.DMA((len(widths), NY)),
        ],
        compiler_params=pltpu.CompilerParams(vmem_limit_bytes=16 * 2**20),
        name="decode",
    )(in_vmem(own), in_vmem(other))


def norm_kernel(gains, _, norm):
    few = norm.shape[0] * LANES // (NY * NX * 2)
    row = lax.broadcasted_iota(jnp.int32, (padded(norm.shape[0]), NY), 0)
    chip = lax.broadcasted_iota(jnp.int32, (padded(norm.shape[0]), NY), 1)
    lane = lax.broadcasted_iota(jnp.int32, (NY, LANES), 1)
    own_y = lax.broadcasted_iota(jnp.int32, (NY, LANES), 0)
    total = jnp.zeros((padded(norm.shape[0]), LANES), jnp.float32)
    for k in range(NX):
        for c in range(2):
            start = lambda y: ((y * NX + lax.rem(k + 2 * y, NX)) * 2 + c) * few
            values = jnp.sum(gains[k, c].astype(jnp.float32), axis=0)
            here = lane >= lax.rem(start(own_y), LANES)
            for j in range(2):
                part = jnp.where(here if j == 0 else ~here, values, 0.0).astype(jnp.bfloat16)
                pick = jnp.where(lax.div(start(chip), LANES) + j == row, 1.0, 0.0)
                total = total + jnp.dot(
                    pick.astype(jnp.bfloat16), part, preferred_element_type=jnp.float32
                )
    norm[...] = total[: norm.shape[0]].astype(norm.dtype)


def gather_norm(few, gains, after):
    return pl.pallas_call(
        norm_kernel,
        out_shape=jax.ShapeDtypeStruct((NY * NX * 2 * few // LANES, LANES), jnp.bfloat16),
        in_specs=[pl.BlockSpec(memory_space=pltpu.VMEM), pl.BlockSpec(memory_space=pltpu.HBM)],
        out_specs=pl.BlockSpec(memory_space=pltpu.VMEM),
        compiler_params=pltpu.CompilerParams(vmem_limit_bytes=4 * 2**20),
        name="gather_norm",
    )(gains, in_hbm(after))


def place(y, x, c):
    return ((y % NY) * NX + x % NX) * 2 + c


SPOTS = [(y, x, c) for y in range(NY) for x in range(NX) for c in range(2)]


def come_from(value, source):
    return lax.ppermute(value, FSDP, [(place(*source(*s)), place(*s)) for s in SPOTS])


def per_device(n_z, *args):
    arrays, norms = args[:9], args[9:]
    rows = arrays[0].shape[0]
    widths = tuple(a.shape[1] for a in arrays[::3])
    *fresh, wire = encode(NY, norms, arrays)
    same_kind = [[place(y, k - 2 * y, c) for y in range(NY)] for c in range(2) for k in range(NX)]
    own = lax.all_to_all(wire, FSDP, 0, 0, axis_index_groups=same_kind, tiled=True)
    up = come_from(own, lambda y, x, c: (y, x + 1 - 2 * c, c))
    down = come_from(own, lambda y, x, c: (y, x - 1 + 2 * c, c))
    side = come_from(own, lambda y, x, c: (y + 1 - 2 * c, x, c))
    used = sum(w // LANES for w in widths) * (rows + PARTS)
    gain = prepare(used, NX * 2 * n_z, own)
    rest = [
        [
            (place(y, k - 2 * y, c) * n_z) + z
            for k in range(NX)
            for c in range(2)
            for z in range(n_z)
        ]
        for y in range(NY)
    ]
    gains = lax.all_to_all(gain, FSDP + (Z,), 0, 0, axis_index_groups=rest, tiled=True)
    gains = gains.reshape(NX, 2, n_z, NY, LANES)
    own = pack((own, up, side, down))
    other = come_from(own, lambda y, x, c: (y, x, 1 - c))

    out = decode(widths, rows, own, other)
    norm = gather_norm(norms[0].shape[0] * n_z, gains, out[3])
    serve = [s.reshape(-1, s.shape[-1]) for s in out[:3]]
    factor = [f.reshape(-1) for f in out[3:]]
    return (*serve, *factor, norm.reshape(-1), *fresh)


def solution(mesh):
    split = Mesh(mesh.devices.reshape(NY, NX, 2, mesh.shape["model"]), (Y, X, C, Z))
    return jax.shard_map(
        functools.partial(per_device, mesh.shape["model"]),
        mesh=split,
        in_specs=(P(FSDP, Z),) * 9 + (P((*FSDP, Z)),) * 2,
        out_specs=(P(None, Z),) * 3 + (P(Z),) * 3 + (P(),) + (P(FSDP, Z),) * 3,
        check_vma=False,
    )
```

```python
import functools

import jax
import jax.numpy as jnp
from jax import lax
from jax.experimental import pallas as pl
from jax.experimental.pallas import tpu as pltpu
from jax.sharding import Mesh
from jax.sharding import PartitionSpec as P


Y, X, C, Z = "fsdp_0", "fsdp_1", "fsdp_2", "model"
FSDP = (Y, X, C)
NY, NX = 8, 4

learn_rate = 0.02
decay_rate = 0.05
tiny_value = 1e-08

LANES = 128
SPAN = 125.0
FLOOR = 1e-28
PARTS = 2


def padded(rows):
    return -(-rows // 8) * 8


def spot():
    return tuple(lax.axis_index(a) for a in (Y, X, C))


def encode_kernel(widths, *refs):
    n = len(widths)
    norms, refs = refs[:2], refs[2:]
    sources, fresh_refs, wire = refs[: 3 * n], refs[3 * n : 4 * n], refs[4 * n]
    ins, (norm_train, norm_step, sems) = refs[4 * n + 1 : -3], refs[-3:]
    loads = [pltpu.make_async_copy(s, d, sems.at[i]) for i, (s, d) in enumerate(zip(sources, ins))]
    few_loads = [
        pltpu.make_async_copy(s, d, sems.at[3 * n + i])
        for i, (s, d) in enumerate(zip(norms, (norm_train, norm_step)))
    ]
    for load in loads + few_loads:
        load.start()
    copies = wire.shape[0]
    rows = ins[0].shape[0]
    slabs = sum(w // LANES for w in widths)
    slab = 0
    for at, width in enumerate(widths):
        train, drift, spread = ins[3 * at : 3 * at + 3]
        for load in loads[3 * at : 3 * at + 3]:
            load.wait()
        for k in range(width // LANES):
            cols = slice(k * LANES, (k + 1) * LANES)
            t = train[:, cols]
            fresh = t - learn_rate * (
                drift[:, cols] / (jnp.sqrt(spread[:, cols]) + tiny_value) + decay_rate * t
            )
            fresh_refs[at][:, cols] = fresh
            left = jnp.maximum(jnp.max(jnp.abs(fresh), axis=0, keepdims=True), FLOOR)
            parts = []
            scale = jnp.zeros_like(left)
            for _ in range(PARTS):
                parts.append(left.astype(jnp.bfloat16))
                part = parts[-1].astype(jnp.float32)
                scale, left = scale + part, left - part
            code = jnp.exp2(fresh * (SPAN / scale)).astype(jnp.bfloat16)
            for c in range(copies):
                wire[c, slab * rows : (slab + 1) * rows, :] = code
                for p, part in enumerate(parts):
                    row = slabs * rows + p * 8 + slab
                    wire[c, row : row + 1, :] = part
            slab += 1
    used = slabs * rows + 7
    few = norm_train.shape[0]
    y, x, c = spot()
    start = (place(y, x, c) * lax.axis_size(Z) + lax.axis_index(Z)) * few
    lane = lax.broadcasted_iota(jnp.int32, (1, LANES), 1) - lax.rem(start, LANES)
    lane = jnp.where(lane < 0, lane + LANES, lane)
    gain = jnp.zeros((1, LANES), jnp.float32)
    for load in few_loads:
        load.wait()
    for i in range(few):
        gain = jnp.where(lane == i, norm_train[i] + norm_step[i], gain)
    gain = gain.astype(jnp.bfloat16)
    for copy in range(copies):
        wire[copy, used : used + 1, :] = gain


def encode(copies, norms, arrays):
    rows = arrays[0].shape[0]
    widths = tuple(a.shape[1] for a in arrays[::3])
    slabs = sum(w // LANES for w in widths)
    out = [pltpu.VMEM(a.shape, a.dtype) for a in arrays[::3]]
    out.append(pltpu.VMEM((copies, slabs * rows + PARTS * 8, LANES), jnp.bfloat16))
    vmem = pl.BlockSpec(memory_space=pltpu.VMEM)
    return pl.pallas_call(
        functools.partial(encode_kernel, widths),
        out_shape=out,
        in_specs=[pl.BlockSpec(memory_space=pltpu.HBM)] * (2 + len(arrays)),
        out_specs=[vmem] * len(out),
        scratch_shapes=[pltpu.VMEM(a.shape, a.dtype) for a in arrays]
        + [pltpu.SMEM(a.shape, a.dtype) for a in norms]
        + [pltpu.SemaphoreType.DMA((len(arrays) + 2,))],
        compiler_params=pltpu.CompilerParams(vmem_limit_bytes=16 * 2**20),
        name="encode",
    )(*(in_hbm(a) for a in norms), *(in_hbm(a) for a in arrays))


def prepare_kernel(row, own, out):
    rows = own[:, row - row % 8 : row - row % 8 + 8, :].astype(jnp.float32)[:, row % 8, :]
    rows = rows.astype(out.dtype)
    for i in range(out.shape[0]):
        out[i] = rows


def prepare(row, copies, own):
    vmem = pl.BlockSpec(memory_space=pltpu.VMEM)
    return pl.pallas_call(
        functools.partial(prepare_kernel, row),
        out_shape=pltpu.VMEM((copies, own.shape[0], LANES), own.dtype),
        in_specs=[vmem],
        out_specs=vmem,
        compiler_params=pltpu.CompilerParams(vmem_limit_bytes=4 * 2**20),
        name="prepare",
    )(in_vmem(own))


def pack_kernel(*refs):
    for i, ref in enumerate(refs[:-1]):
        refs[-1][i] = ref[...]


def pack(arrays):
    vmem = pl.BlockSpec(memory_space=pltpu.VMEM)
    return pl.pallas_call(
        pack_kernel,
        out_shape=pltpu.VMEM((len(arrays), *arrays[0].shape), arrays[0].dtype),
        in_specs=[vmem] * len(arrays),
        out_specs=vmem,
        compiler_params=pltpu.CompilerParams(vmem_limit_bytes=4 * 2**20),
        name="pack",
    )(*(in_vmem(a) for a in arrays))


def in_hbm(value):
    return pltpu.with_memory_space_constraint(value, pltpu.HBM)


def in_vmem(value):
    return pltpu.with_memory_space_constraint(value, pltpu.VMEM)


def decode_kernel(widths, rows, *refs):
    n = len(widths)
    wires = [refs[i // 4].at[i % 4] for i in range(8)]
    refs = refs[2:]
    serve, factor, scratch = refs[:n], refs[n : 2 * n], refs[2 * n :]
    stage, ratios, sems = scratch[:n], scratch[n], scratch[n + 1]
    slabs = sum(w // LANES for w in widths)
    low = slabs * rows
    y, x, mine = spot()
    kind = lax.rem(x + 2 * y, NX)
    best = None
    for i, wire in enumerate(wires):
        scale = wire[:, low : low + 8, :].astype(jnp.float32)
        for p in range(1, PARTS):
            scale = scale + wire[:, low + 8 * p : low + 8 * (p + 1), :].astype(jnp.float32)
        ratios[i] = scale
        top = jnp.max(scale, axis=0)
        best = top if best is None else jnp.maximum(best, top)
    slab = 0
    for at, width in enumerate(widths):
        for k in range(width // LANES):
            factor[at][:, k * LANES : (k + 1) * LANES] = best[slab : slab + 1]
            slab += 1
    share = 1.0 / (SPAN * best)
    for i in range(8):
        ratios[i] = ratios[i] * share

    def copy(at, part):
        return pltpu.make_async_copy(stage[at].at[part], serve[at].at[part], sems.at[at])

    def body(y, _):
        for i, wire in enumerate(wires):
            c = mine if i < 4 else 1 - mine
            x = lax.rem(kind + (0, 1 + 2 * c, 2, 3 - 2 * c)[i % 4] + 2 * y, NX)
            slab = 0
            for at, width in enumerate(widths):
                for k in range(width // LANES):
                    cols = slice(k * LANES, (k + 1) * LANES)
                    code = wire[y, slab * rows : (slab + 1) * rows, :].astype(jnp.float32)
                    ratio = ratios[i, y, slab : slab + 1, :]
                    stage[at][y, x, c, :, cols] = (jnp.log2(code) * ratio).astype(jnp.bfloat16)
                    slab += 1
        for at in range(n):
            copy(at, y).start()
        return 0

    lax.fori_loop(0, NY, body, 0)
    for at in range(n):
        copy(at, slice(None)).wait()


def decode(widths, rows, own, other):
    stage = [(NY, NX, 2, rows, w) for w in widths]
    vmem = pl.BlockSpec(memory_space=pltpu.VMEM)
    out = [jax.ShapeDtypeStruct(s, jnp.bfloat16) for s in stage]
    out += [jax.ShapeDtypeStruct((1, w), jnp.float32) for w in widths]
    return pl.pallas_call(
        functools.partial(decode_kernel, widths, rows),
        out_shape=out,
        in_specs=[vmem] * 2,
        out_specs=[pl.BlockSpec(memory_space=pl.ANY)] * len(widths) + [vmem] * len(widths),
        scratch_shapes=[pltpu.VMEM(s, jnp.bfloat16) for s in stage]
        + [
            pltpu.VMEM((8, NY, 8, LANES), jnp.float32),
            pltpu.SemaphoreType.DMA((len(widths),)),
        ],
        compiler_params=pltpu.CompilerParams(vmem_limit_bytes=16 * 2**20),
        name="decode",
    )(in_vmem(own), in_vmem(other))


def norm_kernel(gains, _, norm):
    few = norm.shape[0] * LANES // (NY * NX * 2)
    row = lax.broadcasted_iota(jnp.int32, (padded(norm.shape[0]), NY), 0)
    chip = lax.broadcasted_iota(jnp.int32, (padded(norm.shape[0]), NY), 1)
    lane = lax.broadcasted_iota(jnp.int32, (NY, LANES), 1)
    own_y = lax.broadcasted_iota(jnp.int32, (NY, LANES), 0)
    total = jnp.zeros((padded(norm.shape[0]), LANES), jnp.float32)
    for k in range(NX):
        for c in range(2):
            start = lambda y: ((y * NX + lax.rem(k + 2 * y, NX)) * 2 + c) * few
            values = jnp.sum(gains[k, c].astype(jnp.float32), axis=0)
            here = lane >= lax.rem(start(own_y), LANES)
            for j in range(2):
                part = jnp.where(here if j == 0 else ~here, values, 0.0).astype(jnp.bfloat16)
                pick = jnp.where(lax.div(start(chip), LANES) + j == row, 1.0, 0.0)
                total = total + jnp.dot(
                    pick.astype(jnp.bfloat16), part, preferred_element_type=jnp.float32
                )
    norm[...] = total[: norm.shape[0]].astype(norm.dtype)


def gather_norm(few, gains, after):
    return pl.pallas_call(
        norm_kernel,
        out_shape=jax.ShapeDtypeStruct((NY * NX * 2 * few // LANES, LANES), jnp.bfloat16),
        in_specs=[pl.BlockSpec(memory_space=pltpu.VMEM), pl.BlockSpec(memory_space=pltpu.HBM)],
        out_specs=pl.BlockSpec(memory_space=pltpu.VMEM),
        compiler_params=pltpu.CompilerParams(vmem_limit_bytes=4 * 2**20),
        name="gather_norm",
    )(gains, in_hbm(after))


def place(y, x, c):
    return ((y % NY) * NX + x % NX) * 2 + c


SPOTS = [(y, x, c) for y in range(NY) for x in range(NX) for c in range(2)]


def come_from(value, source):
    return lax.ppermute(value, FSDP, [(place(*source(*s)), place(*s)) for s in SPOTS])


def per_device(n_z, *args):
    arrays, norms = args[:9], args[9:]
    rows = arrays[0].shape[0]
    widths = tuple(a.shape[1] for a in arrays[::3])
    *fresh, wire = encode(NY, norms, arrays)
    same_kind = [[place(y, k - 2 * y, c) for y in range(NY)] for c in range(2) for k in range(NX)]
    own = lax.all_to_all(wire, FSDP, 0, 0, axis_index_groups=same_kind, tiled=True)
    up = come_from(own, lambda y, x, c: (y, x + 1 - 2 * c, c))
    down = come_from(own, lambda y, x, c: (y, x - 1 + 2 * c, c))
    side = come_from(own, lambda y, x, c: (y + 1 - 2 * c, x, c))
    used = sum(w // LANES for w in widths) * rows + 7
    gain = prepare(used, NX * 2 * n_z, own)
    rest = []
    for y in range(0, NY, 2):
        for x in range(0, NX, 2):
            square = sorted(
                ((x + j + 2 * (y + i)) % NX, y + i, x + j) for i in range(2) for j in range(2)
            )
            rest.append(
                [
                    place(at_y, at_x, c) * n_z + z
                    for _, at_y, at_x in square
                    for c in range(2)
                    for z in range(n_z)
                ]
            )
    gains = lax.all_to_all(gain, FSDP + (Z,), 0, 0, axis_index_groups=rest, tiled=True)
    gains = gains.reshape(NX, 2, n_z, NY, LANES)
    own = pack((own, up, side, down))
    other = come_from(own, lambda y, x, c: (y, x, 1 - c))

    out = decode(widths, rows, own, other)
    norm = gather_norm(norms[0].shape[0] * n_z, gains, out[3])
    serve = [s.reshape(-1, s.shape[-1]) for s in out[:3]]
    factor = [f.reshape(-1) for f in out[3:]]
    return (*serve, *factor, norm.reshape(-1), *fresh)


def solution(mesh):
    split = Mesh(mesh.devices.reshape(NY, NX, 2, mesh.shape["model"]), (Y, X, C, Z))
    return jax.shard_map(
        functools.partial(per_device, mesh.shape["model"]),
        mesh=split,
        in_specs=(P(FSDP, Z),) * 9 + (P((*FSDP, Z)),) * 2,
        out_specs=(P(None, Z),) * 3 + (P(Z),) * 3 + (P(),) + (P(FSDP, Z),) * 3,
        check_vma=False,
    )
```

```python
import functools

import jax
import jax.numpy as jnp
from jax import lax
from jax.experimental import pallas as pl
from jax.experimental.pallas import tpu as pltpu
from jax.sharding import Mesh
from jax.sharding import PartitionSpec as P


Y, X, C, Z = "fsdp_0", "fsdp_1", "fsdp_2", "model"
FSDP = (Y, X, C)
NY, NX = 8, 4

learn_rate = 0.02
decay_rate = 0.05
tiny_value = 1e-08

LANES = 128
SPAN = 125.0
FLOOR = 1e-28
PARTS = 2


def padded(rows):
    return -(-rows // 8) * 8


def spot():
    return tuple(lax.axis_index(a) for a in (Y, X, C))


def encode_kernel(widths, *refs):
    n = len(widths)
    norms, refs = refs[:2], refs[2:]
    sources, fresh_refs, wire = refs[: 3 * n], refs[3 * n : 4 * n], refs[4 * n]
    ins, (norm_train, norm_step, sems) = refs[4 * n + 1 : -3], refs[-3:]
    loads = [pltpu.make_async_copy(s, d, sems.at[i]) for i, (s, d) in enumerate(zip(sources, ins))]
    few_loads = [
        pltpu.make_async_copy(s, d, sems.at[3 * n + i])
        for i, (s, d) in enumerate(zip(norms, (norm_train, norm_step)))
    ]
    for at in sorted(range(n), key=lambda at: widths[at]):
        for load in loads[3 * at : 3 * at + 3]:
            load.start()
    for load in few_loads:
        load.start()
    copies = wire.shape[0]
    rows = ins[0].shape[0]
    slabs = sum(w // LANES for w in widths)
    for at in sorted(range(n), key=lambda at: widths[at]):
        width, slab = widths[at], sum(w // LANES for w in widths[:at])
        train, drift, spread = ins[3 * at : 3 * at + 3]
        for load in loads[3 * at : 3 * at + 3]:
            load.wait()
        for k in range(width // LANES):
            cols = slice(k * LANES, (k + 1) * LANES)
            t = train[:, cols]
            fresh = t - learn_rate * (
                drift[:, cols] / (jnp.sqrt(spread[:, cols]) + tiny_value) + decay_rate * t
            )
            fresh_refs[at][:, cols] = fresh
            left = jnp.maximum(jnp.max(jnp.abs(fresh), axis=0, keepdims=True), FLOOR)
            parts = []
            scale = jnp.zeros_like(left)
            for _ in range(PARTS):
                parts.append(left.astype(jnp.bfloat16))
                part = parts[-1].astype(jnp.float32)
                scale, left = scale + part, left - part
            code = jnp.exp2(fresh * (SPAN / scale)).astype(jnp.bfloat16)
            for c in range(copies):
                wire[c, slab * rows : (slab + 1) * rows, :] = code
                for p, part in enumerate(parts):
                    row = slabs * rows + p * 8 + slab
                    wire[c, row : row + 1, :] = part
            slab += 1
    used = slabs * rows + 7
    few = norm_train.shape[0]
    y, x, c = spot()
    start = (place(y, x, c) * lax.axis_size(Z) + lax.axis_index(Z)) * few
    lane = lax.broadcasted_iota(jnp.int32, (1, LANES), 1) - lax.rem(start, LANES)
    lane = jnp.where(lane < 0, lane + LANES, lane)
    gain = jnp.zeros((1, LANES), jnp.float32)
    for load in few_loads:
        load.wait()
    for i in range(few):
        gain = jnp.where(lane == i, norm_train[i] + norm_step[i], gain)
    gain = gain.astype(jnp.bfloat16)
    for copy in range(copies):
        wire[copy, used : used + 1, :] = gain


def encode(copies, norms, arrays):
    rows = arrays[0].shape[0]
    widths = tuple(a.shape[1] for a in arrays[::3])
    slabs = sum(w // LANES for w in widths)
    out = [pltpu.VMEM(a.shape, a.dtype) for a in arrays[::3]]
    out.append(pltpu.VMEM((copies, slabs * rows + PARTS * 8, LANES), jnp.bfloat16))
    vmem = pl.BlockSpec(memory_space=pltpu.VMEM)
    return pl.pallas_call(
        functools.partial(encode_kernel, widths),
        out_shape=out,
        in_specs=[pl.BlockSpec(memory_space=pltpu.HBM)] * (2 + len(arrays)),
        out_specs=[vmem] * len(out),
        scratch_shapes=[pltpu.VMEM(a.shape, a.dtype) for a in arrays]
        + [pltpu.SMEM(a.shape, a.dtype) for a in norms]
        + [pltpu.SemaphoreType.DMA((len(arrays) + 2,))],
        compiler_params=pltpu.CompilerParams(vmem_limit_bytes=16 * 2**20),
        name="encode",
    )(*(in_hbm(a) for a in norms), *(in_hbm(a) for a in arrays))


def prepare_kernel(row, own, out):
    rows = own[:, row - row % 8 : row - row % 8 + 8, :].astype(jnp.float32)[:, row % 8, :]
    rows = rows.astype(out.dtype)
    for i in range(out.shape[0]):
        out[i] = rows


def prepare(row, copies, own):
    vmem = pl.BlockSpec(memory_space=pltpu.VMEM)
    return pl.pallas_call(
        functools.partial(prepare_kernel, row),
        out_shape=pltpu.VMEM((copies, own.shape[0], LANES), own.dtype),
        in_specs=[vmem],
        out_specs=vmem,
        compiler_params=pltpu.CompilerParams(vmem_limit_bytes=4 * 2**20),
        name="prepare",
    )(in_vmem(own))


def pack_kernel(*refs):
    for i, ref in enumerate(refs[:-1]):
        refs[-1][i] = ref[...]


def pack(arrays):
    vmem = pl.BlockSpec(memory_space=pltpu.VMEM)
    return pl.pallas_call(
        pack_kernel,
        out_shape=pltpu.VMEM((len(arrays), *arrays[0].shape), arrays[0].dtype),
        in_specs=[vmem] * len(arrays),
        out_specs=vmem,
        compiler_params=pltpu.CompilerParams(vmem_limit_bytes=4 * 2**20),
        name="pack",
    )(*(in_vmem(a) for a in arrays))


def in_hbm(value):
    return pltpu.with_memory_space_constraint(value, pltpu.HBM)


def in_vmem(value):
    return pltpu.with_memory_space_constraint(value, pltpu.VMEM)


def decode_kernel(widths, rows, *refs):
    n = len(widths)
    wires = [refs[i // 4].at[i % 4] for i in range(8)]
    refs = refs[2:]
    serve, factor, scratch = refs[:n], refs[n : 2 * n], refs[2 * n :]
    stage, ratios, sems = scratch[:n], scratch[n], scratch[n + 1]
    slabs = sum(w // LANES for w in widths)
    low = slabs * rows
    y, x, mine = spot()
    kind = lax.rem(x + 2 * y, NX)
    best = None
    for i, wire in enumerate(wires):
        scale = wire[:, low : low + 8, :].astype(jnp.float32)
        for p in range(1, PARTS):
            scale = scale + wire[:, low + 8 * p : low + 8 * (p + 1), :].astype(jnp.float32)
        ratios[i] = scale
        top = jnp.max(scale, axis=0)
        best = top if best is None else jnp.maximum(best, top)
    slab = 0
    for at, width in enumerate(widths):
        for k in range(width // LANES):
            factor[at][:, k * LANES : (k + 1) * LANES] = best[slab : slab + 1]
            slab += 1
    share = 1.0 / (SPAN * best)
    for i in range(8):
        ratios[i] = ratios[i] * share

    def copy(at, part):
        return pltpu.make_async_copy(stage[at].at[part], serve[at].at[part], sems.at[at])

    def body(y, _):
        for i, wire in enumerate(wires):
            c = mine if i < 4 else 1 - mine
            x = lax.rem(kind + (0, 1 + 2 * c, 2, 3 - 2 * c)[i % 4] + 2 * y, NX)
            slab = 0
            for at, width in enumerate(widths):
                for k in range(width // LANES):
                    cols = slice(k * LANES, (k + 1) * LANES)
                    code = wire[y, slab * rows : (slab + 1) * rows, :].astype(jnp.float32)
                    ratio = ratios[i, y, slab : slab + 1, :]
                    stage[at][y, x, c, :, cols] = (jnp.log2(code) * ratio).astype(jnp.bfloat16)
                    slab += 1
        for at in range(n):
            copy(at, y).start()
        return 0

    lax.fori_loop(0, NY, body, 0)
    for at in range(n):
        copy(at, slice(None)).wait()


def decode(widths, rows, own, other):
    stage = [(NY, NX, 2, rows, w) for w in widths]
    vmem = pl.BlockSpec(memory_space=pltpu.VMEM)
    out = [jax.ShapeDtypeStruct(s, jnp.bfloat16) for s in stage]
    out += [jax.ShapeDtypeStruct((1, w), jnp.float32) for w in widths]
    return pl.pallas_call(
        functools.partial(decode_kernel, widths, rows),
        out_shape=out,
        in_specs=[vmem] * 2,
        out_specs=[pl.BlockSpec(memory_space=pl.ANY)] * len(widths) + [vmem] * len(widths),
        scratch_shapes=[pltpu.VMEM(s, jnp.bfloat16) for s in stage]
        + [
            pltpu.VMEM((8, NY, 8, LANES), jnp.float32),
            pltpu.SemaphoreType.DMA((len(widths),)),
        ],
        compiler_params=pltpu.CompilerParams(vmem_limit_bytes=16 * 2**20),
        name="decode",
    )(in_vmem(own), in_vmem(other))


def norm_kernel(gains, _, norm):
    few = norm.shape[0] * LANES // (NY * NX * 2)
    row = lax.broadcasted_iota(jnp.int32, (padded(norm.shape[0]), NY), 0)
    chip = lax.broadcasted_iota(jnp.int32, (padded(norm.shape[0]), NY), 1)
    lane = lax.broadcasted_iota(jnp.int32, (NY, LANES), 1)
    own_y = lax.broadcasted_iota(jnp.int32, (NY, LANES), 0)
    total = jnp.zeros((padded(norm.shape[0]), LANES), jnp.float32)
    for k in range(NX):
        for c in range(2):
            start = lambda y: ((y * NX + lax.rem(k + 2 * y, NX)) * 2 + c) * few
            values = jnp.sum(gains[k, c].astype(jnp.float32), axis=0)
            here = lane >= lax.rem(start(own_y), LANES)
            for j in range(2):
                part = jnp.where(here if j == 0 else ~here, values, 0.0).astype(jnp.bfloat16)
                pick = jnp.where(lax.div(start(chip), LANES) + j == row, 1.0, 0.0)
                total = total + jnp.dot(
                    pick.astype(jnp.bfloat16), part, preferred_element_type=jnp.float32
                )
    norm[...] = total[: norm.shape[0]].astype(norm.dtype)


def gather_norm(few, gains, after):
    return pl.pallas_call(
        norm_kernel,
        out_shape=jax.ShapeDtypeStruct((NY * NX * 2 * few // LANES, LANES), jnp.bfloat16),
        in_specs=[pl.BlockSpec(memory_space=pltpu.VMEM), pl.BlockSpec(memory_space=pltpu.HBM)],
        out_specs=pl.BlockSpec(memory_space=pltpu.VMEM),
        compiler_params=pltpu.CompilerParams(vmem_limit_bytes=4 * 2**20),
        name="gather_norm",
    )(gains, in_hbm(after))


def place(y, x, c):
    return ((y % NY) * NX + x % NX) * 2 + c


SPOTS = [(y, x, c) for y in range(NY) for x in range(NX) for c in range(2)]


def come_from(value, source):
    return lax.ppermute(value, FSDP, [(place(*source(*s)), place(*s)) for s in SPOTS])


def per_device(n_z, *args):
    arrays, norms = args[:9], args[9:]
    rows = arrays[0].shape[0]
    widths = tuple(a.shape[1] for a in arrays[::3])
    *fresh, wire = encode(NY, norms, arrays)
    same_kind = [[place(y, k - 2 * y, c) for y in range(NY)] for c in range(2) for k in range(NX)]
    own = lax.all_to_all(wire, FSDP, 0, 0, axis_index_groups=same_kind, tiled=True)
    up = come_from(own, lambda y, x, c: (y, x + 1 - 2 * c, c))
    down = come_from(own, lambda y, x, c: (y, x - 1 + 2 * c, c))
    side = come_from(own, lambda y, x, c: (y - 1 + 2 * c, x, c))
    used = sum(w // LANES for w in widths) * rows + 7
    gain = prepare(used, NX * 2 * n_z, own)
    rest = []
    for y in range(0, NY, 2):
        for x in range(0, NX, 2):
            square = sorted(
                ((x + j + 2 * (y + i)) % NX, y + i, x + j) for i in range(2) for j in range(2)
            )
            rest.append(
                [
                    place(at_y, at_x, c) * n_z + z
                    for _, at_y, at_x in square
                    for c in range(2)
                    for z in range(n_z)
                ]
            )
    gains = lax.all_to_all(gain, FSDP + (Z,), 0, 0, axis_index_groups=rest, tiled=True)
    gains = gains.reshape(NX, 2, n_z, NY, LANES)
    own = pack((own, up, side, down))
    other = come_from(own, lambda y, x, c: (y, x, 1 - c))

    out = decode(widths, rows, own, other)
    norm = gather_norm(norms[0].shape[0] * n_z, gains, out[3])
    serve = [s.reshape(-1, s.shape[-1]) for s in out[:3]]
    factor = [f.reshape(-1) for f in out[3:]]
    return (*serve, *factor, norm.reshape(-1), *fresh)


def solution(mesh):
    split = Mesh(mesh.devices.reshape(NY, NX, 2, mesh.shape["model"]), (Y, X, C, Z))
    return jax.shard_map(
        functools.partial(per_device, mesh.shape["model"]),
        mesh=split,
        in_specs=(P(FSDP, Z),) * 9 + (P((*FSDP, Z)),) * 2,
        out_specs=(P(None, Z),) * 3 + (P(Z),) * 3 + (P(),) + (P(FSDP, Z),) * 3,
        check_vma=False,
    )
```
